32 devices in a mesh: fsdp: 8 (over y, x, core), model: 4 (over z).
Axes of the slice: x: 2, y: 2, z: 4, core: 2. Of those that a mesh axis runs over, the one named last changes fastest.
Arguments:
- w_query: float32 [4096, 4096], P('fsdp', 'model'), may hold values from -0.125 to 0.125
- first_query: float32 [4096, 4096], P('fsdp', 'model'), may hold values from -0.09375 to 0.09375
- second_query: float32 [4096, 4096], P('fsdp', 'model'), may hold values from -0.09375 to 0.09375
- w_key: float32 [4096, 4096], P('fsdp', 'model'), may hold values from -0.125 to 0.125
- first_key: float32 [4096, 4096], P('fsdp', 'model'), may hold values from -0.09375 to 0.09375
- second_key: float32 [4096, 4096], P('fsdp', 'model'), may hold values from -0.09375 to 0.09375
- w_value: float32 [4096, 4096], P('fsdp', 'model'), may hold values from -0.125 to 0.125
- first_value: float32 [4096, 4096], P('fsdp', 'model'), may hold values from -0.09375 to 0.09375
- second_value: float32 [4096, 4096], P('fsdp', 'model'), may hold values from -0.09375 to 0.09375
- norm_gain: float32 [4096], P('fsdp'), may hold values from 0.25 to 1.75
Outputs:
- ready_query: bfloat16 [4096, 4096], P(None, 'model')
- ready_key: bfloat16 [4096, 4096], P(None, 'model')
- ready_value: bfloat16 [4096, 4096], P(None, 'model')
- factor_query: float32 [4096], P('model')
- factor_key: float32 [4096], P('model')
- factor_value: float32 [4096], P('model')
The draws below stay inside these ranges and needn't reach their ends.
All inputs are finite; a program needn't handle non-finite values. Where the reference program divides by a largest or mean magnitude, that divisor is 1e-20 or more.
Results may differ from the reference program's by a relative error of at most 0.001.
Values may be sent and summed in bfloat16 or wider, within the bound.
No kernel may reach another device: no remote copies, remote signals or barrier semaphores. Data moves between devices by JAX's collectives and lax.ppermute only.
A program may use at most 128 MiB of HBM per device.

```python
import jax
import jax.numpy as jnp

D_MODEL = 4096
Q_DIM = 4096
KV_DIM = 4096


def strengthened(values, own_key, source, target, shards_of, factor):
    def block_of(axis_at):
        return (jnp.arange(values.shape[axis_at]) // (values.shape[axis_at] // shards_of)).reshape((-1,) + (1,) * (values.ndim - 1 - axis_at))

    one_side = jax.random.permutation(own_key, shards_of)[block_of(target)]
    far = (block_of(target) + shards_of // 2) % shards_of
    return jnp.where((block_of(source) == one_side) | (block_of(source) == far), factor * values, values)


def levels(key, extent, cuts, low, top_value):
    gain, own = 1.0, jax.random.fold_in(key, 6)
    for position, parts in cuts:
        heights = jnp.exp(jax.random.uniform(jax.random.fold_in(own, position), (parts,), jnp.float32, low / len(cuts), top_value / len(cuts)))
        gain = gain * jnp.repeat(heights, extent[position] // parts).reshape([-1 if axis == position else 1 for axis in range(len(extent))])
    return gain


def centred(own_key, shape, deviation, most, split=(), kind=jnp.bfloat16):
    values = deviation * jax.random.normal(own_key, shape, jnp.float32)
    if split:
        values = values * levels(own_key, shape, split, -0.22, 0.18)
    return jnp.clip(values, -most, most).astype(kind)


def gaussian_with(key, extent, scale, most, pieces, heavy, kind=jnp.bfloat16):
    drawn = scale * jax.random.normal(key, extent, jnp.float32)
    if pieces:
        drawn = drawn * levels(key, extent, pieces, -0.22, 0.18)
    return jnp.clip(strengthened(drawn, jax.random.fold_in(key, 3), *heavy), -most, most).astype(kind)


def setup_inputs(seed: int = 0) -> dict:
    key_of = jax.random.split(jax.random.key(seed), 11)
    return {
        "w_query": gaussian_with(key_of[0], (D_MODEL, Q_DIM), D_MODEL ** -0.5, 0.125, ((0, 8), (1, 4)), (0, 1, 8, 2.0), jnp.float32),
        "first_query": centred(key_of[1], (D_MODEL, Q_DIM), D_MODEL ** -0.5, 0.09375, ((0, 8), (1, 4)), jnp.float32),
        "second_query": centred(key_of[2], (D_MODEL, Q_DIM), D_MODEL ** -0.5, 0.09375, ((0, 8), (1, 4)), jnp.float32),
        "w_key": gaussian_with(key_of[3], (D_MODEL, KV_DIM), D_MODEL ** -0.5, 0.125, ((0, 8), (1, 4)), (0, 1, 8, 2.0), jnp.float32),
        "first_key": centred(key_of[4], (D_MODEL, KV_DIM), D_MODEL ** -0.5, 0.09375, ((0, 8), (1, 4)), jnp.float32),
        "second_key": centred(key_of[5], (D_MODEL, KV_DIM), D_MODEL ** -0.5, 0.09375, ((0, 8), (1, 4)), jnp.float32),
        "w_value": gaussian_with(key_of[6], (D_MODEL, KV_DIM), D_MODEL ** -0.5, 0.125, ((0, 8), (1, 4)), (0, 1, 8, 2.0), jnp.float32),
        "first_value": centred(key_of[7], (D_MODEL, KV_DIM), D_MODEL ** -0.5, 0.09375, ((0, 8), (1, 4)), jnp.float32),
        "second_value": centred(key_of[8], (D_MODEL, KV_DIM), D_MODEL ** -0.5, 0.09375, ((0, 8), (1, 4)), jnp.float32),
        "norm_gain": jnp.clip(1.0 + 0.15 * jax.random.normal(key_of[9], (D_MODEL,), jnp.float32), 0.25, 1.75),
    }


learn_rate = 0.2
hold_rate = 0.9


def reference(w_query, first_query, second_query, w_key, first_key, second_key, w_value, first_value, second_value, norm_gain):
    hold_query = hold_rate * first_query + second_query
    latest_query = w_query - learn_rate * hold_query
    hold_key = hold_rate * first_key + second_key
    latest_key = w_key - learn_rate * hold_key
    hold_value = hold_rate * first_value + second_value
    latest_value = w_value - learn_rate * hold_value
    latest_gained_query = latest_query * norm_gain[:, None]
    latest_gained_key = latest_key * norm_gain[:, None]
    latest_gained_value = latest_value * norm_gain[:, None]
    factor_query = jnp.sum(jnp.abs(latest_gained_query), axis=0) / D_MODEL
    ready_query = (latest_gained_query / factor_query).astype(jnp.bfloat16)
    factor_key = jnp.sum(jnp.abs(latest_gained_key), axis=0) / D_MODEL
    ready_key = (latest_gained_key / factor_key).astype(jnp.bfloat16)
    factor_value = jnp.sum(jnp.abs(latest_gained_value), axis=0) / D_MODEL
    ready_value = (latest_gained_value / factor_value).astype(jnp.bfloat16)
    return ready_query, ready_key, ready_value, factor_query, factor_key, factor_value
```

```python
import jax
import jax.numpy as jnp
from jax import lax
from jax.sharding import PartitionSpec as P

learn_rate = 0.2
hold_rate = 0.9


def swap(value, mask, n):
    return lax.ppermute(value, "fsdp", [(i, i ^ mask) for i in range(n)])


def total_over_fsdp(value, n):
    mask = 1
    while mask < n:
        value = value + swap(value, mask, n)
        mask *= 2
    return value


def latest_gained(w, first, second, norm_gain):
    hold = hold_rate * first + second
    return (w - learn_rate * hold) * norm_gain[:, None]


def gather_rows(blocks, n):
    links = n.bit_length() - 2
    masks = [2 << j for j in range(links)]
    me = lax.axis_index("fsdp")
    rows = blocks[0].shape[0]
    part = rows // links
    outs = [jnp.zeros((n * rows, b.shape[1]), b.dtype) for b in blocks]

    def put(t, offset, start, value):
        at = (me ^ offset) * rows + start
        outs[t] = lax.dynamic_update_slice(outs[t], value, (at, 0))

    first = [[swap(b, m, n) for m in masks] for b in blocks]
    for t, b in enumerate(blocks):
        put(t, 0, 0, b)
        put(t, 1, 0, swap(b, 1, n))
    waiting = []
    for t in range(len(blocks)):
        for j in range(links):
            got = first[t][j]
            for p in range(links):
                at = (j - p) % links
                piece = lax.slice_in_dim(got, p * part, (p + 1) * part)
                waiting.append((t, masks[j], p, at, piece))
    level = waiting
    while level:
        following = []
        for t, offset, p, at, piece in level:
            for step in range(at + 1, links):
                m = masks[(p + step) % links]
                following.append((t, offset ^ m, p, step, swap(piece, m, n)))
        level = following
        waiting = waiting + following
    for t in range(len(blocks)):
        for j in range(links):
            put(t, masks[j], 0, first[t][j])
            put(t, masks[j] ^ 1, 0, swap(first[t][j], 1, n))
    for t, offset, p, at, piece in waiting[len(blocks) * links * links:]:
        put(t, offset, p * part, piece)
        put(t, offset ^ 1, p * part, swap(piece, 1, n))
    return outs


def solution(mesh):
    n = mesh.shape["fsdp"]

    def on_device(wq, fq, sq, wk, fk, sk, wv, fv, sv, norm_gain):
        gained = [
            latest_gained(w, f, s, norm_gain)
            for w, f, s in ((wq, fq, sq), (wk, fk, sk), (wv, fv, sv))
        ]
        part = jnp.stack([jnp.sum(jnp.abs(g), axis=0) for g in gained])
        factor = total_over_fsdp(part, n) / (n * wq.shape[0])
        narrow = [(g / f).astype(jnp.bfloat16) for g, f in zip(gained, factor)]
        ready = gather_rows(narrow, n)
        return (*ready, factor[0], factor[1], factor[2])

    return jax.shard_map(
        on_device,
        mesh=mesh,
        in_specs=(P("fsdp", "model"),) * 9 + (P("fsdp"),),
        out_specs=(P(None, "model"),) * 3 + (P("model"),) * 3,
        check_vma=False,
    )
```

```python
import functools
import math

import jax
import jax.numpy as jnp
from jax import lax
from jax.experimental import pallas as pl
from jax.experimental.pallas import tpu as pltpu
from jax.sharding import PartitionSpec as P


learn_rate = 0.2
hold_rate = 0.9

VMEM_LIMIT = 16 * 1024 * 1024
LANES = 128


def swap(value, mask, n):
    return lax.ppermute(value, "fsdp", [(i, i ^ mask) for i in range(n)])


def hbm(value):
    return pltpu.with_memory_space_constraint(value, pltpu.HBM)


def step_rows(rows):
    return math.gcd(rows, 64)


def gain_columns(gain_ref, start, rows, slab):
    at = start // LANES
    row = jnp.broadcast_to(gain_ref[:, pl.ds(pl.multiple_of(at * LANES, LANES), LANES)], (slab, LANES))
    lane = lax.broadcasted_iota(jnp.int32, (slab, LANES), 1)
    place_of = lax.broadcasted_iota(jnp.int32, (slab, LANES), 0) + (start - at * LANES)
    return [
        jnp.sum(jnp.where(lane == place_of + r, row, 0.0), axis=1, keepdims=True)
        for r in range(0, rows, slab)
    ]


def lane_groups(cols):
    return [slice(at, at + LANES) for at in range(0, cols, LANES)]


def update_kernel(count, chunk, gain_ref, *refs):
    ins, kept, sums = refs[: 3 * count], refs[3 * count : 4 * count], refs[4 * count]
    held, (acc_ref, column_ref, sems) = refs[4 * count + 1 : -3], refs[-3:]
    rows, cols = kept[0].shape
    chunks = rows // chunk

    def copy(c, j):
        at = pl.ds(pl.multiple_of(c * chunk, 8), chunk)
        return pltpu.make_async_copy(ins[j].at[at], held[j].at[at], sems.at[c, j])

    for c in range(chunks):
        for j in range(3 * count):
            copy(c, j).start()
    acc_ref[...] = jnp.zeros_like(acc_ref)
    for start in range(0, rows, chunk):
        for i, column in enumerate(gain_columns(gain_ref, start, chunk, 8)):
            column_ref[start + 8 * i : start + 8 * i + 8, :] = jnp.broadcast_to(column, (8, LANES))

    def work(c, _):
        spots = [pl.ds(pl.multiple_of(c * chunk + r, 8), 8) for r in range(0, chunk, 8)]
        columns = [column_ref[at, :] for at in spots]
        for t in range(count):
            w, first, second = held[3 * t : 3 * t + 3]
            for j in range(3 * t, 3 * t + 3):
                copy(c, j).wait()
            for lanes in lane_groups(cols):
                acc = acc_ref[t, :, lanes]
                for at, column in zip(spots, columns):
                    hold = hold_rate * first[at, lanes] + second[at, lanes]
                    gained = (w[at, lanes] - learn_rate * hold) * column
                    kept[t][at, lanes] = gained
                    acc += jnp.abs(gained)
                acc_ref[t, :, lanes] = acc
        return _

    lax.fori_loop(0, chunks, work, 0)
    for t in range(count):
        sums[t : t + 1, :] = jnp.sum(acc_ref[t], axis=0, keepdims=True)


def update(triples, gain_row):
    rows, cols = triples[0][0].shape
    chunk = step_rows(rows)
    count = len(triples)
    size = rows * cols * count
    *gained, sums = pl.pallas_call(
        functools.partial(update_kernel, count, chunk),
        in_specs=[pl.BlockSpec(memory_space=pltpu.VMEM)]
        + [pl.BlockSpec(memory_space=pltpu.HBM)] * (3 * count),
        out_specs=[pl.BlockSpec(memory_space=pltpu.VMEM)] * (count + 1),
        out_shape=[jax.ShapeDtypeStruct((rows, cols), jnp.float32)] * count
        + [jax.ShapeDtypeStruct((count, cols), jnp.float32)],
        scratch_shapes=[pltpu.VMEM((rows, cols), jnp.float32)] * (3 * count)
        + [
            pltpu.VMEM((count, 8, cols), jnp.float32),
            pltpu.VMEM((rows, LANES), jnp.float32),
            pltpu.SemaphoreType.DMA((rows // chunk, 3 * count)),
        ],
        compiler_params=pltpu.CompilerParams(vmem_limit_bytes=VMEM_LIMIT),
        cost_estimate=pl.CostEstimate(flops=8 * size, bytes_accessed=12 * size, transcendentals=0),
        name="update",
    )(gain_row, *[hbm(a) for triple in triples for a in triple])
    return gained, sums


def mean_of(index, rows_all, me_ref, totals, roles):
    values = [r[index : index + 1, :] for r in totals]
    even = (me_ref[0] & 1) == 0
    if roles == "fast":
        own, got, other, across = values
        values = [own, jnp.where(even, got, other), across, jnp.where(even, other, got)]
    if roles == "aside":
        own, got, other, both, passed = values
        values = [
            own,
            jnp.where(even, got, other),
            jnp.where(even, other, got),
            jnp.where(even, passed, both),
        ]
    while len(values) > 1:
        values = [a + b for a, b in zip(values[::2], values[1::2])]
    return values[0] / rows_all


def narrow_kernel(index, count, rows_all, edges, roles, me_ref, *refs):
    totals, block, pieces = refs[:count], refs[count], refs[count + 1 : -2]
    factor, scale = refs[-2:]
    rows, cols = block.shape
    step = pl.program_id(0)

    @pl.when(step == 0)
    def _():
        mean = mean_of(index, rows_all, me_ref, totals, roles)
        factor[...] = mean
        scale[...] = 1.0 / mean

    def write(piece):
        for lanes in lane_groups(cols):
            by = scale[:, lanes]
            for r in range(0, rows, 16):
                piece[r : r + 16, lanes] = (block[r : r + 16, lanes] * by).astype(jnp.bfloat16)

    for p, piece in enumerate(pieces):
        pl.when((step >= edges[p]) & (step < edges[p + 1]))(functools.partial(write, piece))


def narrow(gained, totals, roles, index, me, n, sizes):
    rows, cols = gained.shape
    br = math.gcd(step_rows(rows), *sizes)
    edges = [sum(sizes[:p]) // br for p in range(len(sizes) + 1)]
    size = rows * cols

    def piece_spec(p):
        return pl.BlockSpec((br, cols), lambda i: (jnp.clip(i - edges[p], 0, edges[p + 1] - edges[p] - 1), 0))

    *pieces, factor = pl.pallas_call(
        functools.partial(narrow_kernel, index, len(totals), float(n * rows), edges, roles),
        grid=(rows // br,),
        in_specs=[pl.BlockSpec(memory_space=pltpu.SMEM)]
        + [pl.BlockSpec(t.shape, lambda i: (0, 0)) for t in totals]
        + [pl.BlockSpec((br, cols), lambda i: (i, 0))],
        out_specs=[piece_spec(p) for p in range(len(sizes))] + [pl.BlockSpec((1, cols), lambda i: (0, 0))],
        out_shape=[jax.ShapeDtypeStruct((s, cols), jnp.bfloat16) for s in sizes]
        + [jax.ShapeDtypeStruct((1, cols), jnp.float32)],
        scratch_shapes=[pltpu.VMEM((1, cols), jnp.float32)],
        compiler_params=pltpu.CompilerParams(vmem_limit_bytes=VMEM_LIMIT),
        cost_estimate=pl.CostEstimate(flops=8 * size, bytes_accessed=6 * size, transcendentals=0),
        name="narrow",
    )(me, *totals, gained)
    return pieces, factor.reshape(cols)


def place_kernel(spots, rows, held, me_ref, *refs):
    pieces, out, sems = refs[held : held + len(spots)], refs[-2], refs[-1]
    copies = []
    for i, (offset, start) in enumerate(spots):
        at = pl.multiple_of((me_ref[0] ^ offset) * rows + start, 16)
        copies.append(
            pltpu.make_async_copy(pieces[i], out.at[pl.ds(at, pieces[i].shape[0])], sems.at[i])
        )
        copies[-1].start()
    for copy in copies:
        copy.wait()


def place(out, me, n, rows, items):
    spots = tuple((offset, start) for offset, start, _ in items)
    pieces = [piece for _, _, piece in items]
    size = sum(piece.size for piece in pieces)
    held = [] if out is None else [out]
    return pl.pallas_call(
        functools.partial(place_kernel, spots, rows, len(held)),
        in_specs=[pl.BlockSpec(memory_space=pltpu.SMEM)]
        + [pl.BlockSpec(memory_space=pltpu.HBM)] * len(held)
        + [pl.BlockSpec(memory_space=pltpu.VMEM)] * len(pieces),
        out_specs=pl.BlockSpec(memory_space=pltpu.HBM),
        out_shape=jax.ShapeDtypeStruct((n * rows, pieces[0].shape[1]), pieces[0].dtype),
        input_output_aliases={1: 0} if held else {},
        scratch_shapes=[pltpu.SemaphoreType.DMA((len(pieces),))],
        compiler_params=pltpu.CompilerParams(vmem_limit_bytes=VMEM_LIMIT),
        cost_estimate=pl.CostEstimate(flops=size, bytes_accessed=4 * size, transcendentals=0),
        name="place",
    )(me, *held, *pieces)


def send(mask, piece, n):
    return swap(piece, mask, n)


def send_first(pieces, plan, masks, n):
    sent = []
    for p, (_, turn) in enumerate(plan):
        for s in range(len(masks)):
            mask = masks[(turn + s) % len(masks)]
            sent.append((mask, p, s, send(mask, pieces[p], n)))
    return sent


def send_onward(first, plan, masks, n):
    later, level = [], first
    while level:
        following = []
        for offset, p, at, piece in level:
            for step in range(at + 1, len(masks)):
                mask = masks[(plan[p][1] + step) % len(masks)]
                following.append((offset ^ mask, p, step, send(mask, piece, n)))
        level = following
        later += level
    return later


def assemble(pieces, first, later, plan, me, n):
    starts = [sum(size for size, _ in plan[:p]) for p in range(len(plan) + 1)]
    stages = [
        [(0, starts[p], x) for p, x in enumerate(pieces)] + [(o, starts[p], x) for o, p, _, x in first],
        [(1, starts[p], send(1, x, n)) for p, x in enumerate(pieces)]
        + [(o ^ 1, starts[p], send(1, x, n)) for o, p, _, x in first],
        [(o, starts[p], x) for o, p, _, x in later],
        [(o ^ 1, starts[p], send(1, x, n)) for o, p, _, x in later],
    ]
    out = None
    for items in stages:
        if items:
            out = place(out, me, n, starts[-1], items)
    return out


def chip_totals(sums, n, aside):
    chip = sums + swap(sums, 1, n)
    if n.bit_length() != 4:
        return [chip] + [swap(chip, 2 * o, n) for o in range(1, n // 2)], "all"
    if aside:
        got = lax.ppermute(chip, "fsdp", [(i, i ^ (4 if i & 1 else 2)) for i in range(n)])
        both = lax.ppermute(chip, "fsdp", [(i, i ^ 6) for i in range(n) if i & 1])
    else:
        got = lax.ppermute(chip, "fsdp", [(i, i ^ (6 if i & 1 else 2)) for i in range(n)])
        across = swap(chip, 4, n)
    other = send(1, got, n)
    if aside:
        return [chip, got, other, both, send(1, both, n)], "aside"
    return [chip, got, other, across], "fast"


def plans_for(rows, links, count):
    if links == 2 and rows % 128 == 0:
        long, half = rows * 5 // 8, rows // 2
        return [[(long, 0), (rows - long, 1)], [(long, 1), (rows - long, 0)], [(half, 0), (half, 1)]]
    return [[(rows // links, p) for p in range(links)]] * count


def solution(mesh):
    n = mesh.shape["fsdp"]
    links = n.bit_length() - 2
    masks = [2 << j for j in range(links)]

    def on_device(wq, fq, sq, wk, fk, sk, wv, fv, sv, norm_gain):
        me = lax.axis_index("fsdp").astype(jnp.int32).reshape(1)
        gain_row = hbm(norm_gain[None, :])
        plans = plans_for(wq.shape[0], links, 3)
        sizes = [[size for size, _ in plan] for plan in plans]
        gained, sums = update([(wq, fq, sq)], gain_row)
        totals, roles = chip_totals(sums, n, False)
        pieces, factor = narrow(gained[0], totals, roles, 0, me, n, sizes[0])
        gained, sums = update([(wk, fk, sk), (wv, fv, sv)], gain_row)
        totals, roles = chip_totals(sums, n, True)
        narrowed = [
            narrow(g, totals, roles, t, me, n, sizes[t + 1]) for t, g in enumerate(gained)
        ]
        pieces = [pieces, narrowed[0][0], narrowed[1][0]]
        outs = []
        for t, plan in enumerate(plans):
            first = send_first(pieces[t], plan, masks, n)
            later = send_onward(first, plan, masks, n)
            outs.append(assemble(pieces[t], first, later, plan, me, n))
        return (*outs, factor, narrowed[0][1], narrowed[1][1])

    return jax.shard_map(
        on_device,
        mesh=mesh,
        in_specs=(P("fsdp", "model"),) * 9 + (P("fsdp"),),
        out_specs=(P(None, "model"),) * 3 + (P("model"),) * 3,
        check_vma=False,
    )
```

```python
import functools
import math

import jax
import jax.numpy as jnp
from jax import lax
from jax.experimental import pallas as pl
from jax.experimental.pallas import tpu as pltpu
from jax.sharding import PartitionSpec as P


learn_rate = 0.2
hold_rate = 0.9

VMEM_LIMIT = 16 * 1024 * 1024
LANES = 128


def swap(value, mask, n):
    return lax.ppermute(value, "fsdp", [(i, i ^ mask) for i in range(n)])


def hbm(value):
    return pltpu.with_memory_space_constraint(value, pltpu.HBM)


def step_rows(rows):
    return math.gcd(rows, 64)


def gain_columns(gain_ref, start, rows, slab):
    at = start // LANES
    row = jnp.broadcast_to(gain_ref[:, pl.ds(pl.multiple_of(at * LANES, LANES), LANES)], (slab, LANES))
    lane = lax.broadcasted_iota(jnp.int32, (slab, LANES), 1)
    place_of = lax.broadcasted_iota(jnp.int32, (slab, LANES), 0) + (start - at * LANES)
    return [
        jnp.sum(jnp.where(lane == place_of + r, row, 0.0), axis=1, keepdims=True)
        for r in range(0, rows, slab)
    ]


def lane_groups(cols):
    return [slice(at, at + LANES) for at in range(0, cols, LANES)]


def update_kernel(count, chunk, gain_ref, *refs):
    ins, kept, sums = refs[: 3 * count], refs[3 * count : 4 * count], refs[4 * count]
    held, (acc_ref, column_ref, sems) = refs[4 * count + 1 : -3], refs[-3:]
    rows, cols = kept[0].shape
    chunks = rows // chunk

    def copy(c, j):
        at = pl.ds(pl.multiple_of(c * chunk, 8), chunk)
        return pltpu.make_async_copy(ins[j].at[at], held[j].at[at], sems.at[c, j])

    for c in range(chunks):
        for j in range(3 * count):
            copy(c, j).start()
    acc_ref[...] = jnp.zeros_like(acc_ref)
    for start in range(0, rows, chunk):
        for i, column in enumerate(gain_columns(gain_ref, start, chunk, 8)):
            column_ref[start + 8 * i : start + 8 * i + 8, :] = jnp.broadcast_to(column, (8, LANES))

    def work(c, _):
        spots = [pl.ds(pl.multiple_of(c * chunk + r, 8), 8) for r in range(0, chunk, 8)]
        columns = [column_ref[at, :] for at in spots]
        for t in range(count):
            w, first, second = held[3 * t : 3 * t + 3]
            for j in range(3 * t, 3 * t + 3):
                copy(c, j).wait()
            for lanes in lane_groups(cols):
                acc = acc_ref[t, :, lanes]
                for at, column in zip(spots, columns):
                    hold = hold_rate * first[at, lanes] + second[at, lanes]
                    gained = (w[at, lanes] - learn_rate * hold) * column
                    kept[t][at, lanes] = gained
                    acc += jnp.abs(gained)
                acc_ref[t, :, lanes] = acc
        return _

    lax.fori_loop(0, chunks, work, 0)
    for t in range(count):
        sums[t : t + 1, :] = jnp.sum(acc_ref[t], axis=0, keepdims=True)


def update(triples, gain_row):
    rows, cols = triples[0][0].shape
    chunk = step_rows(rows)
    count = len(triples)
    size = rows * cols * count
    *gained, sums = pl.pallas_call(
        functools.partial(update_kernel, count, chunk),
        in_specs=[pl.BlockSpec(memory_space=pltpu.VMEM)]
        + [pl.BlockSpec(memory_space=pltpu.HBM)] * (3 * count),
        out_specs=[pl.BlockSpec(memory_space=pltpu.VMEM)] * (count + 1),
        out_shape=[jax.ShapeDtypeStruct((rows, cols), jnp.float32)] * count
        + [jax.ShapeDtypeStruct((count, cols), jnp.float32)],
        scratch_shapes=[pltpu.VMEM((rows, cols), jnp.float32)] * (3 * count)
        + [
            pltpu.VMEM((count, 8, cols), jnp.float32),
            pltpu.VMEM((rows, LANES), jnp.float32),
            pltpu.SemaphoreType.DMA((rows // chunk, 3 * count)),
        ],
        compiler_params=pltpu.CompilerParams(vmem_limit_bytes=VMEM_LIMIT),
        cost_estimate=pl.CostEstimate(flops=8 * size, bytes_accessed=12 * size, transcendentals=0),
        name="update",
    )(gain_row, *[hbm(a) for triple in triples for a in triple])
    return gained, sums


def mean_of(index, rows_all, me_ref, totals, roles):
    values = [r[index : index + 1, :] for r in totals]
    even = (me_ref[0] & 1) == 0
    if roles == "fast":
        own, got, other, across = values
        values = [own, jnp.where(even, got, other), across, jnp.where(even, other, got)]
    if roles == "aside":
        own, got, other, both, passed = values
        values = [
            own,
            jnp.where(even, got, other),
            jnp.where(even, other, got),
            jnp.where(even, passed, both),
        ]
    while len(values) > 1:
        values = [a + b for a, b in zip(values[::2], values[1::2])]
    return values[0] / rows_all


def narrow_kernel(index, count, rows_all, start, roles, me_ref, *refs):
    totals, block, pieces, factor = refs[:count], refs[count], refs[count + 1 : -1], refs[-1]
    mean = mean_of(index, rows_all, me_ref, totals, roles)
    factor[...] = mean
    scale = 1.0 / mean
    for piece in pieces:
        rows, cols = piece.shape

        def work(i, _, piece=piece, start=start, cols=cols):
            for lanes in lane_groups(cols):
                x = block[pl.ds(pl.multiple_of(start + i * 16, 16), 16), lanes]
                piece[pl.ds(pl.multiple_of(i * 16, 16), 16), lanes] = (x * scale[:, lanes]).astype(jnp.bfloat16)
            return _

        lax.fori_loop(0, rows // 16, work, 0, unroll=2 if rows % 32 == 0 else 1)
        start += rows


def narrow(gained, totals, roles, index, me, n, start, sizes):
    rows, cols = gained.shape
    size = sum(sizes) * cols
    *pieces, factor = pl.pallas_call(
        functools.partial(narrow_kernel, index, len(totals), float(n * rows), start, roles),
        in_specs=[pl.BlockSpec(memory_space=pltpu.SMEM)]
        + [pl.BlockSpec(memory_space=pltpu.VMEM)] * (len(totals) + 1),
        out_specs=[pl.BlockSpec(memory_space=pltpu.VMEM)] * (len(sizes) + 1),
        out_shape=[jax.ShapeDtypeStruct((s, cols), jnp.bfloat16) for s in sizes]
        + [jax.ShapeDtypeStruct((1, cols), jnp.float32)],
        compiler_params=pltpu.CompilerParams(vmem_limit_bytes=VMEM_LIMIT),
        cost_estimate=pl.CostEstimate(flops=8 * size, bytes_accessed=6 * size, transcendentals=0),
        name="narrow",
    )(me, *totals, gained)
    return pieces, factor.reshape(cols)


def mask_of(link, core, links):
    return 2 << ((link + core) % links)


def place_kernel(spots, rows, held, me_ref, *refs):
    pieces, out, sems = refs[held : held + len(spots)], refs[-2], refs[-1]
    me = me_ref[0]
    copies = []
    for i, (even, odd, start) in enumerate(spots):
        device = me ^ jnp.where((me & 1) == 0, even, odd)
        at = pl.multiple_of(device * rows + start, 16)
        copies.append(
            pltpu.make_async_copy(pieces[i], out.at[pl.ds(at, pieces[i].shape[0])], sems.at[i])
        )
        copies[-1].start()
    for copy in copies:
        copy.wait()


def place(out, me, n, rows, items):
    spots = tuple(item[:3] for item in items)
    pieces = [item[3] for item in items]
    size = sum(piece.size for piece in pieces)
    held = [] if out is None else [out]
    return pl.pallas_call(
        functools.partial(place_kernel, spots, rows, len(held)),
        in_specs=[pl.BlockSpec(memory_space=pltpu.SMEM)]
        + [pl.BlockSpec(memory_space=pltpu.HBM)] * len(held)
        + [pl.BlockSpec(memory_space=pltpu.VMEM)] * len(pieces),
        out_specs=pl.BlockSpec(memory_space=pltpu.HBM),
        out_shape=jax.ShapeDtypeStruct((n * rows, pieces[0].shape[1]), pieces[0].dtype),
        input_output_aliases={1: 0} if held else {},
        scratch_shapes=[pltpu.SemaphoreType.DMA((len(pieces),))],
        compiler_params=pltpu.CompilerParams(vmem_limit_bytes=VMEM_LIMIT),
        cost_estimate=pl.CostEstimate(flops=size, bytes_accessed=4 * size, transcendentals=0),
        name="place",
    )(me, *held, *pieces)


def over_link(link, piece, n, links):
    pairs = [(i, i ^ mask_of(link, i & 1, links)) for i in range(n)]
    return lax.ppermute(piece, "fsdp", pairs)


def to_core(piece, n):
    return swap(piece, 1, n)


def send_first(pieces, plan, n, links):
    sent = []
    for p, (_, turn) in enumerate(plan):
        for s in range(links):
            link = (turn + s) % links
            sent.append(((link,), p, s, over_link(link, pieces[p], n, links)))
    return sent


def send_onward(first, plan, n, links):
    later, level = [], first
    while level:
        following = []
        for crossed, p, at, piece in level:
            for step in range(at + 1, links):
                link = (plan[p][1] + step) % links
                got = over_link(link, piece, n, links)
                following.append((crossed + (link,), p, step, got))
        level = following
        later += level
    return later


def assemble(pieces, first, later, plan, me, n, links, last):
    starts = [sum(size for size, _ in plan[:p]) for p in range(len(plan) + 1)]

    def own(crossed, p, piece):
        even, odd = (sum(mask_of(link, core, links) for link in crossed) for core in (0, 1))
        return even, odd, starts[p], piece

    def near(crossed, p, piece):
        even, odd, start, _ = own(crossed, p, piece)
        return odd ^ 1, even ^ 1, start, to_core(piece, n)

    stages = [
        [own((), p, x) for p, x in enumerate(pieces)] + [own(c, p, x) for c, p, _, x in first],
        [near((), p, x) for p, x in enumerate(pieces)]
        + [near(c, p, x) for c, p, _, x in first],
    ]
    batches = [later]
    if len(plan) > links:
        split = len(plan) - links
        batches = [[x for x in later if x[1] < split], [x for x in later if x[1] >= split]]
    for b, batch in enumerate(batches):
        mine = [own(c, p, x) for c, p, _, x in batch]
        others = [near(c, p, x) for c, p, _, x in batch]
        stages += [mine, others] if last and b == len(batches) - 1 else [mine + others]
    out = None
    for items in stages:
        if items:
            out = place(out, me, n, starts[-1], items)
    return out


def chip_totals(sums, n, aside):
    chip = sums + swap(sums, 1, n)
    if n.bit_length() != 4:
        return [chip] + [swap(chip, 2 * o, n) for o in range(1, n // 2)], "all"
    if aside:
        got = lax.ppermute(chip, "fsdp", [(i, i ^ (4 if i & 1 else 2)) for i in range(n)])
        both = lax.ppermute(chip, "fsdp", [(i, i ^ 6) for i in range(n) if i & 1])
    else:
        got = lax.ppermute(chip, "fsdp", [(i, i ^ (6 if i & 1 else 2)) for i in range(n)])
        across = swap(chip, 4, n)
    other = to_core(got, n)
    if aside:
        return [chip, got, other, both, to_core(both, n)], "aside"
    return [chip, got, other, across], "fast"


def plans_for(rows, links, count):
    if links == 2 and count == 3 and rows % 256 == 0:
        unit = rows // 16
        return [
            [(10 * unit, 0), (6 * unit, 1)],
            [(10 * unit, 1), (6 * unit, 0)],
            [(5 * unit, 0), (5 * unit, 1), (3 * unit, 0), (3 * unit, 1)],
        ]
    return [[(rows // links, p) for p in range(links)]] * count


def solution(mesh):
    n = mesh.shape["fsdp"]
    links = n.bit_length() - 2

    def on_device(wq, fq, sq, wk, fk, sk, wv, fv, sv, norm_gain):
        me = lax.axis_index("fsdp").astype(jnp.int32).reshape(1)
        gain_row = hbm(norm_gain[None, :])
        plans = plans_for(wq.shape[0], links, 3)
        sizes = [[size for size, _ in plan] for plan in plans]
        gained, sums = update([(wq, fq, sq)], gain_row)
        totals, roles = chip_totals(sums, n, False)
        head, factor = narrow(gained[0], totals, roles, 0, me, n, 0, sizes[0][:1])
        rest, _ = narrow(gained[0], totals, roles, 0, me, n, sizes[0][0], sizes[0][1:])
        gained, sums = update([(wk, fk, sk), (wv, fv, sv)], gain_row)
        totals, roles = chip_totals(sums, n, True)
        narrowed = [
            narrow(g, totals, roles, t, me, n, 0, sizes[t + 1]) for t, g in enumerate(gained)
        ]
        pieces = [head + rest, narrowed[0][0], narrowed[1][0]]
        outs = []
        for t, plan in enumerate(plans):
            first = send_first(pieces[t], plan, n, links)
            later = send_onward(first, plan, n, links)
            outs.append(assemble(pieces[t], first, later, plan, me, n, links, t == 2))
        return (*outs, factor, narrowed[0][1], narrowed[1][1])

    return jax.shard_map(
        on_device,
        mesh=mesh,
        in_specs=(P("fsdp", "model"),) * 9 + (P("fsdp"),),
        out_specs=(P(None, "model"),) * 3 + (P("model"),) * 3,
        check_vma=False,
    )
```

```python
import functools
import math

import jax
import jax.numpy as jnp
from jax import lax
from jax.experimental import pallas as pl
from jax.experimental.pallas import tpu as pltpu
from jax.sharding import PartitionSpec as P


learn_rate = 0.2
hold_rate = 0.9

VMEM_LIMIT = 16 * 1024 * 1024
LANES = 128


def swap(value, mask, n):
    return lax.ppermute(value, "fsdp", [(i, i ^ mask) for i in range(n)])


def hbm(value):
    return pltpu.with_memory_space_constraint(value, pltpu.HBM)


def step_rows(rows):
    return math.gcd(rows, 64)


def gain_columns(gain_ref, start, rows, slab):
    at = start // LANES
    row = jnp.broadcast_to(gain_ref[:, pl.ds(pl.multiple_of(at * LANES, LANES), LANES)], (slab, LANES))
    lane = lax.broadcasted_iota(jnp.int32, (slab, LANES), 1)
    place_of = lax.broadcasted_iota(jnp.int32, (slab, LANES), 0) + (start - at * LANES)
    return [
        jnp.sum(jnp.where(lane == place_of + r, row, 0.0), axis=1, keepdims=True)
        for r in range(0, rows, slab)
    ]


def lane_groups(cols):
    return [slice(at, at + LANES) for at in range(0, cols, LANES)]


def update_kernel(count, chunk, tails, gain_hbm, *refs):
    ins, kept, sums = refs[: 3 * count], refs[3 * count : 4 * count], refs[4 * count]
    held, (acc_ref, column_ref, gain_ref, sems, gain_sem) = refs[4 * count + 1 + tails : -5], refs[-5:]
    rows, cols = kept[0].shape
    chunks = rows // chunk

    def copy(c, j):
        at = pl.ds(pl.multiple_of(c * chunk, 8), chunk)
        return pltpu.make_async_copy(ins[j].at[at], held[j].at[at], sems.at[c, j])

    gain_copy = pltpu.make_async_copy(gain_hbm, gain_ref, gain_sem)
    gain_copy.start()
    for c in range(chunks):
        for j in range(3 * count):
            copy(c, j).start()
    acc_ref[...] = jnp.zeros_like(acc_ref)
    gain_copy.wait()
    for start in range(0, rows, chunk):
        for i, column in enumerate(gain_columns(gain_ref, start, chunk, 8)):
            column_ref[start + 8 * i : start + 8 * i + 8, :] = jnp.broadcast_to(column, (8, LANES))

    def work(c, _):
        spots = [pl.ds(pl.multiple_of(c * chunk + r, 8), 8) for r in range(0, chunk, 8)]
        columns = [column_ref[at, :] for at in spots]
        for t in range(count):
            w, first, second = held[3 * t : 3 * t + 3]
            for j in range(3 * t, 3 * t + 3):
                copy(c, j).wait()
            for lanes in lane_groups(cols):
                acc = acc_ref[t, :, lanes]
                for at, column in zip(spots, columns):
                    hold = hold_rate * first[at, lanes] + second[at, lanes]
                    gained = (w[at, lanes] - learn_rate * hold) * column
                    kept[t][at, lanes] = gained
                    acc += jnp.abs(gained)
                acc_ref[t, :, lanes] = acc
        return _

    lax.fori_loop(0, chunks, work, 0)
    for t in range(count):
        sums[t : t + 1, :] = jnp.sum(acc_ref[t], axis=0, keepdims=True)
    if tails:
        tail = refs[4 * count + 1]
        tail[...] = kept[0][rows - tail.shape[0] :, :]


def update(triples, gain_row, tail=0):
    rows, cols = triples[0][0].shape
    chunk = step_rows(rows)
    count = len(triples)
    size = rows * cols * count
    tails = 1 if tail else 0
    outs = pl.pallas_call(
        functools.partial(update_kernel, count, chunk, tails),
        in_specs=[pl.BlockSpec(memory_space=pltpu.HBM)] * (3 * count + 1),
        out_specs=[pl.BlockSpec(memory_space=pltpu.VMEM)] * (count + 1 + tails),
        out_shape=[jax.ShapeDtypeStruct((rows, cols), jnp.float32)] * count
        + [jax.ShapeDtypeStruct((count, cols), jnp.float32)]
        + [jax.ShapeDtypeStruct((tail, cols), jnp.float32)] * tails,
        scratch_shapes=[pltpu.VMEM((rows, cols), jnp.float32)] * (3 * count)
        + [
            pltpu.VMEM((count, 8, cols), jnp.float32),
            pltpu.VMEM((rows, LANES), jnp.float32),
            pltpu.VMEM((1, rows), jnp.float32),
            pltpu.SemaphoreType.DMA((rows // chunk, 3 * count)),
            pltpu.SemaphoreType.DMA,
        ],
        compiler_params=pltpu.CompilerParams(vmem_limit_bytes=VMEM_LIMIT),
        cost_estimate=pl.CostEstimate(flops=8 * size, bytes_accessed=12 * size, transcendentals=0),
        name="update",
    )(gain_row, *[hbm(a) for triple in triples for a in triple])
    return outs[:count], outs[count], *outs[count + 1 :]


def mean_of(index, rows_all, totals, roles):
    values = [r[index : index + 1, :] for r in totals]
    even = (lax.axis_index("fsdp") & 1) == 0
    if roles == "fast":
        own, got, other, across = values
        values = [own, jnp.where(even, got, other), across, jnp.where(even, other, got)]
    if roles == "aside":
        own, got, other, both, passed = values
        values = [
            own,
            jnp.where(even, got, other),
            jnp.where(even, other, got),
            jnp.where(even, passed, both),
        ]
    while len(values) > 1:
        values = [a + b for a, b in zip(values[::2], values[1::2])]
    return values[0] / rows_all


def narrow_kernel(index, count, rows_all, start, roles, *refs):
    totals, block, pieces = refs[:count], refs[count], refs[count + 1 :]
    scale = 1.0 / mean_of(index, rows_all, totals, roles)
    for piece in pieces:
        rows, cols = piece.shape

        slab = math.gcd(rows, 64)

        def work(i, _, piece=piece, start=start, cols=cols, slab=slab):
            for lanes in lane_groups(cols):
                by = jnp.broadcast_to(scale[:, lanes], (16, LANES))
                for r in range(0, slab, 16):
                    x = block[pl.ds(pl.multiple_of(start + i * slab + r, 16), 16), lanes]
                    at = pl.ds(pl.multiple_of(i * slab + r, 16), 16)
                    piece[at, lanes] = (x * by).astype(jnp.bfloat16)
            return _

        lax.fori_loop(0, rows // slab, work, 0)
        start += rows


def narrow(gained, totals, roles, index, rows_all, start, sizes):
    cols = gained.shape[1]
    size = sum(sizes) * cols
    return list(pl.pallas_call(
        functools.partial(narrow_kernel, index, len(totals), float(rows_all), start, roles),
        in_specs=[pl.BlockSpec(memory_space=pltpu.VMEM)] * (len(totals) + 1),
        out_specs=[pl.BlockSpec(memory_space=pltpu.VMEM)] * len(sizes),
        out_shape=[jax.ShapeDtypeStruct((s, cols), jnp.bfloat16) for s in sizes],
        compiler_params=pltpu.CompilerParams(vmem_limit_bytes=VMEM_LIMIT),
        cost_estimate=pl.CostEstimate(flops=8 * size, bytes_accessed=6 * size, transcendentals=0),
        name="narrow",
    )(*totals, gained))


def factors_kernel(rows_all, roles, *refs):
    totals, outs = refs[: -refs[0].shape[0]], refs[-refs[0].shape[0] :]
    for index, out in enumerate(outs):
        out[...] = mean_of(index, rows_all, totals, roles)


def factors(totals, roles, rows_all):
    count, cols = totals[0].shape
    outs = pl.pallas_call(
        functools.partial(factors_kernel, float(rows_all), roles),
        in_specs=[pl.BlockSpec(memory_space=pltpu.VMEM)] * len(totals),
        out_specs=[pl.BlockSpec(memory_space=pltpu.VMEM)] * count,
        out_shape=[jax.ShapeDtypeStruct((1, cols), jnp.float32)] * count,
        compiler_params=pltpu.CompilerParams(vmem_limit_bytes=VMEM_LIMIT),
        cost_estimate=pl.CostEstimate(flops=cols, bytes_accessed=4 * cols, transcendentals=0),
        name="factors",
    )(*totals)
    return [out.reshape(cols) for out in outs]


def mask_of(link, core, links):
    return 2 << ((link + core) % links)


def place_kernel(spots, rows, held, *refs):
    pieces, out, sems = refs[held : held + len(spots)], refs[-2], refs[-1]
    me = lax.axis_index("fsdp")
    copies = []
    for i, (even, odd, start) in enumerate(spots):
        device = me ^ jnp.where((me & 1) == 0, even, odd)
        at = pl.multiple_of(device * rows + start, 16)
        copies.append(
            pltpu.make_async_copy(pieces[i], out.at[pl.ds(at, pieces[i].shape[0])], sems.at[i])
        )
        copies[-1].start()
    for copy in copies:
        copy.wait()


def place(out, n, rows, items):
    spots = tuple(item[:3] for item in items)
    pieces = [item[3] for item in items]
    size = sum(piece.size for piece in pieces)
    held = [] if out is None else [out]
    return pl.pallas_call(
        functools.partial(place_kernel, spots, rows, len(held)),
        in_specs=[pl.BlockSpec(memory_space=pltpu.HBM)] * len(held)
        + [pl.BlockSpec(memory_space=pltpu.VMEM)] * len(pieces),
        out_specs=pl.BlockSpec(memory_space=pltpu.HBM),
        out_shape=jax.ShapeDtypeStruct((n * rows, pieces[0].shape[1]), pieces[0].dtype),
        input_output_aliases={0: 0} if held else {},
        scratch_shapes=[pltpu.SemaphoreType.DMA((len(pieces),))],
        compiler_params=pltpu.CompilerParams(vmem_limit_bytes=VMEM_LIMIT),
        cost_estimate=pl.CostEstimate(flops=size, bytes_accessed=4 * size, transcendentals=0),
        name="place",
    )(*held, *pieces)


def over_link(link, piece, n, links):
    pairs = [(i, i ^ mask_of(link, i & 1, links)) for i in range(n)]
    return lax.ppermute(piece, "fsdp", pairs)


def to_core(piece, n):
    return swap(piece, 1, n)


def send_first(pieces, plan, n, links, arrived):
    sent = []
    for p, (_, turn) in enumerate(plan):
        for s in range(links):
            link = (turn + s) % links
            got = arrived[p][link] if p in arrived else over_link(link, pieces[p], n, links)
            sent.append(((link,), p, s, got))
    return sent


def send_onward(first, plan, n, links):
    later, level = [], first
    while level:
        following = []
        for crossed, p, at, piece in level:
            for step in range(at + 1, links):
                link = (plan[p][1] + step) % links
                got = over_link(link, piece, n, links)
                following.append((crossed + (link,), p, step, got))
        level = following
        later += level
    return later


def assemble(pieces, first, later, plan, n, links, last):
    starts = [sum(size for size, _ in plan[:p]) for p in range(len(plan) + 1)]

    def own(crossed, p, piece):
        even, odd = (sum(mask_of(link, core, links) for link in crossed) for core in (0, 1))
        return even, odd, starts[p], piece

    def near(crossed, p, piece):
        even, odd, start, _ = own(crossed, p, piece)
        return odd ^ 1, even ^ 1, start, to_core(piece, n)

    stages = [
        [own((), p, x) for p, x in enumerate(pieces)] + [own(c, p, x) for c, p, _, x in first],
        [near((), p, x) for p, x in enumerate(pieces)]
        + [near(c, p, x) for c, p, _, x in first],
    ]
    batches = [later]
    if last and len(plan) > links:
        split = len(plan) - links
        batches = [[x for x in later if x[1] < split], [x for x in later if x[1] >= split]]
    for b, batch in enumerate(batches):
        mine = [own(c, p, x) for c, p, _, x in batch]
        others = [near(c, p, x) for c, p, _, x in batch]
        stages += [mine, others] if last and b == len(batches) - 1 else [mine + others]
    out = None
    for items in stages:
        if items:
            out = place(out, n, starts[-1], items)
    return out


def chip_totals(sums, n, aside):
    chip = sums + swap(sums, 1, n)
    if n.bit_length() != 4:
        return [chip] + [swap(chip, 2 * o, n) for o in range(1, n // 2)], "all"
    if aside:
        got = lax.ppermute(chip, "fsdp", [(i, i ^ (4 if i & 1 else 2)) for i in range(n)])
        both = lax.ppermute(chip, "fsdp", [(i, i ^ 6) for i in range(n) if i & 1])
    else:
        got = lax.ppermute(chip, "fsdp", [(i, i ^ (6 if i & 1 else 2)) for i in range(n)])
        across = swap(chip, 4, n)
    other = to_core(got, n)
    if aside:
        return [chip, got, other, both, to_core(both, n)], "aside"
    return [chip, got, other, across], "fast"


def plans_for(rows, links, count):
    if links == 2 and count == 3 and rows % 256 == 0:
        unit = rows // 16
        return [
            [(10 * unit, 0), (5 * unit, 1), (unit, 1)],
            [(10 * unit, 1), (6 * unit, 0)],
            [(5 * unit, 0), (5 * unit, 1), (3 * unit, 0), (3 * unit, 1)],
        ], True
    return [[(rows // links, p) for p in range(links)]] * count, False


def solution(mesh):
    n = mesh.shape["fsdp"]
    links = n.bit_length() - 2

    def on_device(wq, fq, sq, wk, fk, sk, wv, fv, sv, norm_gain):
        rows = wq.shape[0]
        gain_row = hbm(norm_gain[None, :])
        plans, early = plans_for(rows, links, 3)
        sizes = [[size for size, _ in plan] for plan in plans]
        arrived = {}
        gained, sums, *tail = update([(wq, fq, sq)], gain_row, sizes[0][-1] if early else 0)
        totals, roles = chip_totals(sums, n, False)
        if early:
            raw = [over_link(link, tail[0], n, links) for link in range(links)]
        head = narrow(gained[0], totals, roles, 0, n * rows, 0, sizes[0][:1])
        rest = narrow(gained[0], totals, roles, 0, n * rows, sizes[0][0], sizes[0][1:])
        if early:
            arrived[len(plans[0]) - 1] = [narrow(x, totals, roles, 0, n * rows, 0, sizes[0][-1:])[0] for x in raw]
        mean = factors(totals, roles, n * rows)
        gained, sums = update([(wk, fk, sk), (wv, fv, sv)], gain_row)
        totals, roles = chip_totals(sums, n, True)
        narrowed = [
            narrow(g, totals, roles, t, n * rows, 0, sizes[t + 1]) for t, g in enumerate(gained)
        ]
        mean += factors(totals, roles, n * rows)
        pieces = [head + rest, *narrowed]
        outs = []
        for t, plan in enumerate(plans):
            first = send_first(pieces[t], plan, n, links, arrived if t == 0 else {})
            later = send_onward(first, plan, n, links)
            outs.append(assemble(pieces[t], first, later, plan, n, links, t == 2))
        return (*outs, *mean)

    return jax.shard_map(
        on_device,
        mesh=mesh,
        in_specs=(P("fsdp", "model"),) * 9 + (P("fsdp"),),
        out_specs=(P(None, "model"),) * 3 + (P("model"),) * 3,
        check_vma=False,
    )
```
